32 devices in a mesh: row: 4 (over z), head: 8 (over y, x, core).
Axes of the slice: x: 2, y: 2, z: 4, core: 2. Of those that a mesh axis runs over, the one named last changes fastest.
Arguments:
- q_nope: bfloat16 [512, 16384], P('row', 'head'), may hold values from -6 to 6
- q_rope: bfloat16 [512, 8192], P('row', 'head'), may hold values from -192 to 192
- latent_keys: bfloat16 [512, 1024], P(None, 'row'), may hold values from -6 to 6
- rope_keys: bfloat16 [64, 1024], P(None, 'row'), may hold values from -8 to 8
- panel_block: int32 [4], replicated, may hold values from 0 to 15, as said below
- query_pos: int32 [512], P('row'), may hold values from 1 to 4095
- w_uk: bfloat16 [128, 128, 512], P('head'), may hold values from -0.5 to 0.5
- w_uv: bfloat16 [128, 512, 128], P('head'), may hold values from -1 to 1
- w_out: bfloat16 [7168, 16384], P('row', 'head'), may hold values from -0.09375 to 0.09375
Outputs:
- attn_out: bfloat16 [512, 7168], P(('row', 'head'))
The draws below stay inside these ranges and needn't reach their ends.
Inputs may be any that keep to these rules, and one draw needn't show every extreme that they name: `panel_block`: distinct block numbers; 0 and the largest allowed block are always among them.
All inputs are finite; a program needn't handle non-finite values.
Results may differ from the reference program's by a relative error of at most 0.025.
Values may be sent and summed in bfloat16 or wider, within the bound.
No kernel may reach another device: no remote copies, remote signals or barrier semaphores. Data moves between devices by JAX's collectives and lax.ppermute only.
A program may use at most 64 MiB of HBM per device.

```python
import jax
import jax.numpy as jnp
from jax import lax

D = 7168
HEADS = 128
NOPE = 128
ROPE = 64
LATENT = 512
VHEAD = 128
PANEL = 256
QROWS = 512
CACHE = 1024
N_ROW = 4


def draw_q_rope(key, part):
    sample = jax.random.truncated_normal(jax.random.fold_in(key, 17), -6.0, 6.0, (QROWS, HEADS * ROPE), jnp.float32)
    return sample.astype(jnp.bfloat16)


def draw_rope_keys(key, part):
    sample = jax.random.truncated_normal(jax.random.fold_in(key, 29), -6.0, 6.0, (ROPE, CACHE), jnp.float32)
    return sample.astype(jnp.bfloat16)


def draw_panel_block(key, part):
    middle = jax.random.permutation(jax.random.fold_in(key, 71), 4 * N_ROW - 2)[:N_ROW - 2] + 1
    ends = jnp.array([0, 4 * N_ROW - 1], jnp.int32)
    chosen = jnp.concatenate((ends, middle.astype(jnp.int32)))
    order = jax.random.permutation(jax.random.fold_in(key, 73), N_ROW)
    return chosen[order].astype(jnp.int32)


def set_ends(drawn, rng, smallest, top_value):
    shape = drawn.shape
    spot = [jax.random.randint(jax.random.fold_in(rng, axis), (), 0, shape[axis]) for axis in range(len(shape))]
    drawn = drawn.at[tuple(spot)].set(smallest)
    longest = shape.index(max(shape))
    spot[longest] = (spot[longest] + 1) % shape[longest]
    return drawn.at[tuple(spot)].set(top_value)


def steps_of(own_key, extent, pieces, smallest, largest):
    def one(dim, blocks):
        steps = jax.random.uniform(jax.random.fold_in(jax.random.fold_in(own_key, 6), dim), (blocks,), jnp.float32, smallest / len(pieces), largest / len(pieces))
        return jnp.repeat(jnp.exp(steps), extent[dim] // blocks).reshape((-1,) + (1,) * (len(extent) - dim - 1))

    loudness = one(*pieces[0])
    for cut in pieces[1:]:
        loudness = loudness * one(*cut)
    return loudness


def gaussian(stream_key, extent, width, bound, pieces=(), held_as=jnp.bfloat16):
    values = width * jax.random.normal(stream_key, extent, jnp.float32)
    if pieces:
        values = values * steps_of(stream_key, extent, pieces, -0.22, 0.18)
    return jnp.clip(values, -bound, bound).astype(held_as)


def setup_inputs(seed: int = 0) -> dict:
    streams_of = jax.random.split(jax.random.key(seed), 10)
    return {
        "q_nope": gaussian(streams_of[0], (QROWS, HEADS * NOPE), 1.0, 6.0, ((0, 4), (1, 8))),
        "q_rope": draw_q_rope(jax.random.fold_in(streams_of[9], 71), 0),
        "latent_keys": gaussian(streams_of[2], (LATENT, CACHE), 1.0, 6.0, ((1, 4),)),
        "rope_keys": draw_rope_keys(jax.random.fold_in(streams_of[9], 71), 0),
        "panel_block": draw_panel_block(jax.random.fold_in(streams_of[9], 71), 0),
        "query_pos": set_ends(jax.random.randint(streams_of[5], (QROWS,), 1, 4 * CACHE), jax.random.fold_in(streams_of[5], 1), 1, (4 * CACHE) - 1).astype(jnp.int32),
        "w_uk": gaussian(streams_of[6], (HEADS, NOPE, LATENT), NOPE ** -0.5, 0.5, ((0, 8),)),
        "w_uv": gaussian(streams_of[7], (HEADS, LATENT, VHEAD), (LATENT // 16) ** -0.5, 1.0, ((0, 8),)),
        "w_out": gaussian(streams_of[8], (D, HEADS * VHEAD), (HEADS * VHEAD // 4) ** -0.5, 0.09375, ((0, 4), (1, 8))),
    }


softmax_scale = 192.0 ** -0.5


def reference(q_nope, q_rope, latent_keys, rope_keys, panel_block, query_pos, w_uk, w_uv, w_out):
    columns = jnp.arange(CACHE, dtype=jnp.int32)
    key_pos = (panel_block[columns // PANEL] * PANEL + columns % PANEL).astype(jnp.int32)
    visible = key_pos[None, :] <= query_pos[:, None]
    nope_heads = jnp.transpose(q_nope.reshape(QROWS, HEADS, NOPE), (1, 0, 2))
    rope_heads = jnp.transpose(q_rope.reshape(QROWS, HEADS, ROPE), (1, 0, 2))

    def one_head(operands):
        query_nope, query_rope, absorb, expand = operands
        query_latent = jnp.dot(query_nope, absorb, preferred_element_type=jnp.float32).astype(jnp.bfloat16)
        scores = jnp.dot(query_latent, latent_keys, preferred_element_type=jnp.float32)
        scores = scores + jnp.dot(query_rope, rope_keys, preferred_element_type=jnp.float32)
        scores = jnp.where(visible, scores * softmax_scale, -jnp.inf)
        row_max = jnp.max(scores, axis=1, keepdims=True)
        weights = jnp.exp(scores - row_max)
        denominator = jnp.sum(weights, axis=1, keepdims=True)
        summed = jnp.dot(weights.astype(jnp.bfloat16), latent_keys.T, preferred_element_type=jnp.float32)
        mixed_latent = (summed / denominator).astype(jnp.bfloat16)
        return jnp.dot(mixed_latent, expand, preferred_element_type=jnp.float32).astype(jnp.bfloat16)

    head_values = lax.map(one_head, (nope_heads, rope_heads, w_uk, w_uv))
    values = jnp.transpose(head_values, (1, 0, 2)).reshape(QROWS, HEADS * VHEAD)
    return jnp.dot(values, w_out.T, preferred_element_type=jnp.float32).astype(jnp.bfloat16)
```

```python
import jax
import jax.numpy as jnp
from jax import lax
from jax.sharding import PartitionSpec as P

NOPE = 128
ROPE = 64
LATENT = 512
VHEAD = 128
PANEL = 256


softmax_scale = 192.0 ** (-0.5)


def swap(x, axis, mask):
    count = lax.axis_size(axis)
    return lax.ppermute(x, axis, [(i, i ^ mask) for i in range(count)])


def gather_blocks(own):
    count = lax.axis_size("row")
    blocks = {0: own}
    mask = count // 2
    while mask:
        for k in list(blocks):
            blocks[k ^ mask] = swap(blocks[k], "row", mask)
        mask //= 2
    return [blocks[k] for k in range(count)]


def scatter_sum(partial):
    mask = 1
    me = lax.axis_index("head")
    while partial.shape[0] > 1:
        pairs = partial.reshape((partial.shape[0] // 2, 2) + partial.shape[1:])
        bit = jnp.where(me & mask, 1, 0)
        sent = lax.dynamic_index_in_dim(pairs, 1 - bit, 1, keepdims=False).astype(jnp.bfloat16)
        kept = lax.dynamic_index_in_dim(pairs, bit, 1, keepdims=False)
        partial = kept + swap(sent, "head", mask).astype(jnp.float32)
        mask *= 2
    return partial[0]


def on_device(q_nope, q_rope, latent_keys, rope_keys, panel_block, query_pos, w_uk, w_uv, w_out):
    row_count = q_nope.shape[0]
    head_count = w_uk.shape[0]
    row_devices = lax.axis_size("row")
    head_devices = lax.axis_size("head")
    my_row = lax.axis_index("row")
    my_head = lax.axis_index("head")
    sub_rows = row_count // head_devices
    feature_slice = w_out.shape[0]
    half = PANEL // 2

    panel = jnp.concatenate((latent_keys, rope_keys), axis=0)
    side = my_head & 1
    mine = lax.dynamic_slice_in_dim(panel, side * half, half, axis=1)
    halves = gather_blocks(mine)
    stacked = jnp.stack(halves)
    other = swap(stacked, "head", 1)
    keys = jnp.concatenate(halves + [other[k] for k in range(row_devices)], axis=1)
    offsets = jnp.arange(half, dtype=jnp.int32)
    starts = [panel_block[my_row ^ k] * PANEL for k in range(row_devices)]
    key_pos = jnp.concatenate(
        [s + side * half + offsets for s in starts] + [s + (1 - side) * half + offsets for s in starts]
    )

    nope_heads = q_nope.reshape(row_count, head_count, NOPE)
    query_latent = jnp.einsum(
        "rhn,hnl->hrl", nope_heads, w_uk, preferred_element_type=jnp.float32
    ).astype(jnp.bfloat16)
    query_latent = query_latent.reshape(head_count * row_count, LATENT)
    query_rope = jnp.transpose(q_rope.reshape(row_count, head_count, ROPE), (1, 0, 2)).reshape(
        head_count * row_count, ROPE
    )
    flat_pos = jnp.tile(query_pos, head_count)
    latents, ropes = keys[:LATENT], keys[LATENT:]
    scores = jnp.dot(query_latent, latents, preferred_element_type=jnp.float32)
    scores = scores + jnp.dot(query_rope, ropes, preferred_element_type=jnp.float32)
    visible = key_pos[None, :] <= flat_pos[:, None]
    scores = jnp.where(visible, scores * softmax_scale, -jnp.inf)
    top = jnp.max(scores, axis=1)
    weights = jnp.exp(scores - top[:, None])
    denominator = jnp.sum(weights, axis=1)
    summed = lax.dot_general(
        weights.astype(jnp.bfloat16),
        latents,
        (((1,), (1,)), ((), ())),
        preferred_element_type=jnp.float32,
    )
    mixed_latent = (
        (summed / denominator[:, None])
        .astype(jnp.bfloat16)
        .reshape(head_count, row_count, LATENT)
    )
    values = jnp.einsum(
        "hrl,hlv->rhv", mixed_latent, w_uv, preferred_element_type=jnp.float32
    ).astype(jnp.bfloat16)
    values = values.reshape(row_count, head_count * VHEAD)

    blocks = gather_blocks(values)
    out = jnp.zeros((sub_rows, row_devices * feature_slice), jnp.bfloat16)
    for k in range(row_devices):
        partial = lax.dot_general(
            blocks[k], w_out, (((1,), (1,)), ((), ())), preferred_element_type=jnp.float32
        )
        partial = partial.reshape(head_devices, sub_rows, feature_slice)
        piece = scatter_sum(partial).astype(jnp.bfloat16)
        if k:
            piece = swap(piece, "row", k)
        out = lax.dynamic_update_slice(out, piece, (0, (my_row ^ k) * feature_slice))
    return out


def solution(mesh):
    return jax.shard_map(
        on_device,
        mesh=mesh,
        in_specs=(
            P("row", "head"),
            P("row", "head"),
            P(None, "row"),
            P(None, "row"),
            P(),
            P("row"),
            P("head", None, None),
            P("head", None, None),
            P("row", "head"),
        ),
        out_specs=P(("row", "head"), None),
        check_vma=False,
    )
```

```python
import functools

import jax
import jax.numpy as jnp
from jax import lax
from jax.experimental import pallas as pl
from jax.experimental.pallas import tpu as pltpu
from jax.sharding import PartitionSpec as P


NOPE = 128
ROPE = 64
LATENT = 512
VHEAD = 128
PANEL = 256


softmax_scale = 192.0 ** (-0.5)


def in_hbm(x):
    return pltpu.with_memory_space_constraint(x, pltpu.HBM)


def swap(x, axis, mask):
    count = lax.axis_size(axis)
    return lax.ppermute(x, axis, [(i, i ^ mask) for i in range(count)])


def gather_blocks(own):
    count = lax.axis_size("row")
    blocks = {0: own}
    mask = count // 2
    while mask:
        for k in list(blocks):
            moved = []
            for chunk in blocks[k]:
                moved.append(swap(chunk, "row", mask))
            blocks[k ^ mask] = moved
        mask //= 2
    return [blocks[k] for k in range(count)]


def half_kernel(latent_ref, rope_ref, out_ref, sems):
    half = out_ref.shape[1]
    side = lax.axis_index("head") & 1
    columns = pl.ds(pl.multiple_of(side * half, half), half)
    latent = pltpu.make_async_copy(latent_ref.at[:, columns], out_ref.at[:LATENT], sems.at[0])
    rope = pltpu.make_async_copy(rope_ref.at[:, columns], out_ref.at[LATENT:], sems.at[1])
    latent.start()
    rope.start()
    latent.wait()
    rope.wait()


def panel_half(latent_keys, rope_keys):
    half = latent_keys.shape[1] // 2
    depth = LATENT + ROPE
    whole = pl.BlockSpec(memory_space=pltpu.HBM)
    return pl.pallas_call(
        half_kernel,
        in_specs=[whole, whole],
        out_specs=pl.BlockSpec(memory_space=pltpu.VMEM),
        out_shape=jax.ShapeDtypeStruct((depth, half), jnp.bfloat16),
        scratch_shapes=[pltpu.SemaphoreType.DMA((2,))],
        compiler_params=pltpu.CompilerParams(vmem_limit_bytes=2 * 1024 * 1024),
        cost_estimate=pl.CostEstimate(flops=1000000, bytes_accessed=4 * depth * half, transcendentals=0),
        name="panel_half",
    )(in_hbm(latent_keys), in_hbm(rope_keys))


def load_kernel(hbm_ref, out_ref, sem):
    copy = pltpu.make_async_copy(hbm_ref, out_ref, sem)
    copy.start()
    copy.wait()


def load(x):
    return pl.pallas_call(
        load_kernel,
        in_specs=[pl.BlockSpec(memory_space=pltpu.HBM)],
        out_specs=pl.BlockSpec(memory_space=pltpu.VMEM),
        out_shape=pltpu.VMEM(x.shape, x.dtype),
        scratch_shapes=[pltpu.SemaphoreType.DMA],
        compiler_params=pltpu.CompilerParams(vmem_limit_bytes=1024 * 1024 + 2 * x.size),
        cost_estimate=pl.CostEstimate(flops=4000000, bytes_accessed=2 * x.size, transcendentals=0),
        name="load",
    )(in_hbm(x))


def query_kernel(heads, nope_ref, absorb_ref, out_ref):
    for h in range(heads):
        out_ref[h] = jnp.dot(
            nope_ref[:, h * NOPE : (h + 1) * NOPE], absorb_ref[h], preferred_element_type=jnp.float32
        ).astype(jnp.bfloat16)


def queries(q_nope, w_uk):
    rows = q_nope.shape[0]
    head_count = w_uk.shape[0]
    heads = min(4, head_count)
    return pl.pallas_call(
        functools.partial(query_kernel, heads),
        grid=(head_count // heads,),
        in_specs=[
            pl.BlockSpec((rows, heads * NOPE), lambda i: (0, i)),
            pl.BlockSpec((heads, NOPE, LATENT), lambda i: (i, 0, 0)),
        ],
        out_specs=pl.BlockSpec((heads, rows, LATENT), lambda i: (i, 0, 0)),
        out_shape=jax.ShapeDtypeStruct((head_count, rows, LATENT), jnp.bfloat16),
        compiler_params=pltpu.CompilerParams(vmem_limit_bytes=6 * 1024 * 1024),
        cost_estimate=pl.CostEstimate(
            flops=2 * head_count * rows * NOPE * LATENT, bytes_accessed=6 * 1024 * 1024, transcendentals=0
        ),
        name="queries",
    )(in_hbm(q_nope), in_hbm(w_uk))


def assemble_kernel(*refs):
    tile_refs, out_ref = refs[:-1], refs[-1]
    half = tile_refs[0].shape[1]
    for t, tile_ref in enumerate(tile_refs):
        out_ref[:, t * half : (t + 1) * half] = tile_ref[...]


def assemble(tiles):
    depth, half = tiles[0].shape
    vmem = pl.BlockSpec(memory_space=pltpu.VMEM)
    return pl.pallas_call(
        assemble_kernel,
        in_specs=[vmem] * len(tiles),
        out_specs=vmem,
        out_shape=jax.ShapeDtypeStruct((depth, half * len(tiles)), jnp.bfloat16),
        compiler_params=pltpu.CompilerParams(vmem_limit_bytes=4 * 1024 * 1024),
        cost_estimate=pl.CostEstimate(
            flops=1000000, bytes_accessed=4 * depth * half * len(tiles), transcendentals=0
        ),
        name="assemble",
    )(*tiles)


def attention_kernel(
    heads, chunk, block_ref, pos_ref, latent_ref, rope_ref, up_ref, keys_ref, out_ref, limit_ref
):
    half = PANEL // 2
    tiles = keys_ref.shape[1] // half
    rows = limit_ref.shape[0]
    my_row = lax.axis_index("row")
    side = lax.axis_index("head") & 1

    @pl.when(pl.program_id(0) == 0)
    def _():
        across = lax.broadcasted_iota(jnp.int32, (rows, rows), 1)
        down = lax.broadcasted_iota(jnp.int32, (rows, rows), 0)
        pos = pos_ref[:, chunk * rows : (chunk + 1) * rows]
        limit_ref[...] = jnp.sum(jnp.where(across == down, pos, 0), axis=1, keepdims=True)

    lane = lax.broadcasted_iota(jnp.int32, (1, half), 1)
    limit = limit_ref[...]
    shown = []
    for t in range(tiles):
        start = block_ref[my_row ^ (t % (tiles // 2))] * PANEL
        start = start + (side if t < tiles // 2 else 1 - side) * half
        shown.append(start + lane <= limit)
    group = max(1, min(heads, 256 // rows))
    for first in range(0, heads, group):
        query = latent_ref[first : first + group].reshape(group * rows, LATENT)
        rope = jnp.concatenate(
            [rope_ref[:, (first + g) * ROPE : (first + g + 1) * ROPE] for g in range(group)], axis=0
        )
        scores = jnp.dot(query, keys_ref[:LATENT], preferred_element_type=jnp.float32)
        scores = scores + jnp.dot(rope, keys_ref[LATENT:], preferred_element_type=jnp.float32)
        masked = []
        for t in range(tiles):
            part = scores[:, t * half : (t + 1) * half].reshape(group, rows, half)
            masked.append(jnp.where(shown[t][None], part, -jnp.inf).reshape(group * rows, half))
        scores = jnp.concatenate(masked, axis=1)
        top = jnp.max(scores, axis=1, keepdims=True)
        weights = jnp.exp2((scores - top) * (softmax_scale * 1.4426950408889634))
        denominator = jnp.sum(weights, axis=1, keepdims=True)
        mixed = lax.dot_general(
            weights.astype(jnp.bfloat16),
            keys_ref[:LATENT],
            (((1,), (1,)), ((), ())),
            preferred_element_type=jnp.float32,
        )
        mixed = (mixed / denominator).astype(jnp.bfloat16)
        for g in range(group):
            value = jnp.dot(
                mixed[g * rows : (g + 1) * rows], up_ref[first + g], preferred_element_type=jnp.float32
            )
            out_ref[:, (first + g) * VHEAD : (first + g + 1) * VHEAD] = value.astype(jnp.bfloat16)


def attention(panel_block, query_pos, query_latent, q_rope, w_uv, keys, chunk, chunks):
    head_count, all_rows, _ = query_latent.shape
    rows = all_rows // chunks
    heads = min(4, head_count)
    depth, cache = keys.shape
    flops = 2 * head_count * rows * (cache * (depth + LATENT) + LATENT * VHEAD)
    whole = lambda i: (0, 0)
    return pl.pallas_call(
        functools.partial(attention_kernel, heads, chunk),
        grid=(head_count // heads,),
        in_specs=[
            pl.BlockSpec(memory_space=pltpu.SMEM),
            pl.BlockSpec((1, all_rows), whole),
            pl.BlockSpec((heads, rows, LATENT), lambda i: (i, chunk, 0)),
            pl.BlockSpec((rows, heads * ROPE), lambda i: (chunk, i)),
            pl.BlockSpec((heads, LATENT, VHEAD), lambda i: (i, 0, 0)),
            pl.BlockSpec(memory_space=pltpu.VMEM),
        ],
        out_specs=pl.BlockSpec((rows, heads * VHEAD), lambda i: (0, i)),
        out_shape=jax.ShapeDtypeStruct((rows, head_count * VHEAD), jnp.bfloat16),
        scratch_shapes=[pltpu.VMEM((rows, 1), jnp.int32)],
        compiler_params=pltpu.CompilerParams(vmem_limit_bytes=16 * 1024 * 1024),
        cost_estimate=pl.CostEstimate(
            flops=flops, bytes_accessed=8 * 1024 * 1024, transcendentals=head_count * rows * cache
        ),
        name="attention",
    )(panel_block, query_pos.reshape(1, all_rows), query_latent, q_rope, in_hbm(w_uv), keys)


def project_kernel(sub, parts, blocks, *refs):
    values_refs, (w_ref, sent_ref, kept_ref) = refs[:parts], refs[parts:]
    upper = (lax.axis_index("head") & 1) == 1
    features = w_ref.shape[0]
    tiles = [slice(first, min(first + 256, features)) for first in range(0, features, 256)]
    values = jnp.concatenate([r[...] for r in values_refs], axis=0) if parts > 1 else values_refs[0][...]
    for tile in tiles:
        product = lax.dot_general(
            values, w_ref[tile], (((1,), (1,)), ((), ())), preferred_element_type=jnp.float32
        )
        pairs = product.reshape(blocks, -1, 2, sub, product.shape[1])
        kept_ref[:, :, :, tile] = jnp.where(upper, pairs[:, :, 1], pairs[:, :, 0])
        sent_ref[:, :, :, tile] = jnp.where(upper, pairs[:, :, 0], pairs[:, :, 1]).astype(jnp.bfloat16)


def project(blocks, w_out, sub):
    parts = [chunk for block in blocks for chunk in block]
    rows = sum(chunk.shape[0] for chunk in blocks[0])
    features, depth = w_out.shape
    shape = (len(blocks), rows // (2 * sub), sub, features)
    vmem = pl.BlockSpec(memory_space=pltpu.VMEM)
    return pl.pallas_call(
        functools.partial(project_kernel, sub, len(parts), len(blocks)),
        in_specs=[vmem] * (len(parts) + 1),
        out_specs=[vmem, vmem],
        compiler_params=pltpu.CompilerParams(vmem_limit_bytes=(1 + len(blocks)) * 1024 * 1024),
        out_shape=[jax.ShapeDtypeStruct(shape, jnp.bfloat16), jax.ShapeDtypeStruct(shape, jnp.float32)],
        cost_estimate=pl.CostEstimate(
            flops=2 * len(blocks) * rows * depth * features,
            bytes_accessed=2 * depth * (features + rows),
            transcendentals=0,
        ),
        name="project",
    )(*parts, w_out)


def pair_kernel(kept_ref, come_ref, *out_refs):
    chip = lax.axis_index("head") >> 1
    for j, out_ref in enumerate(out_refs):
        at = chip ^ j
        total = kept_ref[:, pl.ds(at, 1)] + come_ref[:, pl.ds(at, 1)].astype(jnp.float32)
        out_ref[...] = total[:, 0].astype(out_ref.dtype)


def pair_sum(kept, come):
    blocks, count, sub, features = kept.shape
    vmem = pl.BlockSpec(memory_space=pltpu.VMEM)
    return pl.pallas_call(
        pair_kernel,
        in_specs=[vmem, vmem],
        out_specs=[vmem] * count,
        compiler_params=pltpu.CompilerParams(vmem_limit_bytes=2 * 1024 * 1024),
        out_shape=[
            jax.ShapeDtypeStruct((blocks, sub, features), jnp.bfloat16 if j else jnp.float32)
            for j in range(count)
        ],
        cost_estimate=pl.CostEstimate(
            flops=blocks * count * sub * features,
            bytes_accessed=6 * blocks * count * sub * features,
            transcendentals=0,
        ),
        name="pair_sum",
    )(kept, come)


def chip_kernel(*refs):
    count = refs[0].shape[0]
    terms, outs = refs[:-count], refs[-count:]
    for b, out_ref in enumerate(outs):
        total = terms[0][b]
        for term in terms[1:]:
            total = total + term[b].astype(jnp.float32)
        out_ref[...] = total.astype(jnp.bfloat16)


def chip_sum(terms):
    blocks, sub, features = terms[0].shape
    vmem = pl.BlockSpec(memory_space=pltpu.VMEM)
    return pl.pallas_call(
        chip_kernel,
        in_specs=[vmem] * len(terms),
        out_specs=[vmem] * blocks,
        compiler_params=pltpu.CompilerParams(vmem_limit_bytes=2 * 1024 * 1024),
        out_shape=[jax.ShapeDtypeStruct((sub, features), jnp.bfloat16)] * blocks,
        cost_estimate=pl.CostEstimate(
            flops=len(terms) * blocks * sub * features,
            bytes_accessed=2 * len(terms) * blocks * sub * features,
            transcendentals=0,
        ),
        name="chip_sum",
    )(*terms)


def finish_kernel(*refs):
    pieces, out_ref = refs[:-1], refs[-1]
    width = pieces[0].shape[1]
    my_row = lax.axis_index("row")
    for k, piece_ref in enumerate(pieces):
        columns = pl.ds(pl.multiple_of((my_row ^ k) * width, width), width)
        out_ref[:, columns] = piece_ref[...]


def finish(pieces):
    sub, width = pieces[0].shape
    if width % 128:
        out = jnp.zeros((sub, width * len(pieces)), jnp.bfloat16)
        for k, piece in enumerate(pieces):
            out = lax.dynamic_update_slice(out, piece, (0, (lax.axis_index("row") ^ k) * width))
        return out
    vmem = pl.BlockSpec(memory_space=pltpu.VMEM)
    return pl.pallas_call(
        finish_kernel,
        in_specs=[vmem] * len(pieces),
        out_specs=vmem,
        compiler_params=pltpu.CompilerParams(vmem_limit_bytes=2 * 1024 * 1024),
        out_shape=jax.ShapeDtypeStruct((sub, width * len(pieces)), jnp.bfloat16),
        name="finish",
    )(*pieces)


def on_device(q_nope, q_rope, latent_keys, rope_keys, panel_block, query_pos, w_uk, w_uv, w_out):
    row_devices = lax.axis_size("row")
    sub_rows = q_nope.shape[0] // lax.axis_size("head")

    mine = panel_half(latent_keys, rope_keys)
    halves = [block[0] for block in gather_blocks([mine])]
    others = [swap(h, "head", 1) for h in halves]
    query_latent = queries(q_nope, w_uk)
    keys = assemble(halves + others)
    chunks = 2
    values = []
    for c in range(chunks):
        values.append(attention(panel_block, query_pos, query_latent, q_rope, w_uv, keys, c, chunks))

    blocks = gather_blocks(values)
    w_out = load(w_out)
    pieces = []
    groups = [list(range(row_devices - 1)), [row_devices - 1]]
    for group in groups:
        sent, kept = project([blocks[k] for k in group], w_out, sub_rows)
        sums = pair_sum(kept, swap(sent, "head", 1))
        terms = [sums[0]]
        for j in range(1, len(sums)):
            terms.append(swap(sums[j], "head", 2 * j))
        for k, total in zip(group, chip_sum(terms)):
            pieces.append(swap(total, "row", k) if k else total)
    return finish(pieces)


def solution(mesh):
    return jax.shard_map(
        on_device,
        mesh=mesh,
        in_specs=(
            P("row", "head"),
            P("row", "head"),
            P(None, "row"),
            P(None, "row"),
            P(),
            P("row"),
            P("head", None, None),
            P("head", None, None),
            P("row", "head"),
        ),
        out_specs=P(("row", "head"), None),
        check_vma=False,
    )
```

```python
import functools

import jax
import jax.numpy as jnp
from jax import lax
from jax.experimental import pallas as pl
from jax.experimental.pallas import tpu as pltpu
from jax.sharding import PartitionSpec as P


NOPE = 128
ROPE = 64
LATENT = 512
VHEAD = 128
PANEL = 256


softmax_scale = 192.0 ** (-0.5)


def in_hbm(x):
    return pltpu.with_memory_space_constraint(x, pltpu.HBM)


def swap(x, axis, mask):
    count = lax.axis_size(axis)
    return lax.ppermute(x, axis, [(i, i ^ mask) for i in range(count)])


def gather_blocks(own, made=None):
    made = made or {}
    count = lax.axis_size("row")
    blocks = {0: own}
    mask = count // 2
    while mask:
        for k in list(blocks):
            known = list(made.get(mask, ())) if k == 0 else []
            moved = []
            for chunk in blocks[k][: len(blocks[k]) - len(known)]:
                moved.append(swap(chunk, "row", mask))
            blocks[k ^ mask] = moved + known
        mask //= 2
    return [blocks[k] for k in range(count)]


def half_kernel(latent_ref, rope_ref, out_ref, sems):
    half = out_ref.shape[1]
    side = lax.axis_index("head") & 1
    columns = pl.ds(pl.multiple_of(side * half, half), half)
    latent = pltpu.make_async_copy(latent_ref.at[:, columns], out_ref.at[:LATENT], sems.at[0])
    rope = pltpu.make_async_copy(rope_ref.at[:, columns], out_ref.at[LATENT:], sems.at[1])
    latent.start()
    rope.start()
    latent.wait()
    rope.wait()


def panel_half(latent_keys, rope_keys):
    half = latent_keys.shape[1] // 2
    depth = LATENT + ROPE
    whole = pl.BlockSpec(memory_space=pltpu.HBM)
    return pl.pallas_call(
        half_kernel,
        in_specs=[whole, whole],
        out_specs=pl.BlockSpec(memory_space=pltpu.VMEM),
        out_shape=jax.ShapeDtypeStruct((depth, half), jnp.bfloat16),
        scratch_shapes=[pltpu.SemaphoreType.DMA((2,))],
        compiler_params=pltpu.CompilerParams(vmem_limit_bytes=2 * 1024 * 1024),
        cost_estimate=pl.CostEstimate(flops=1000000, bytes_accessed=4 * depth * half, transcendentals=0),
        name="panel_half",
    )(in_hbm(latent_keys), in_hbm(rope_keys))


def load_kernel(hbm_ref, out_ref, sem):
    copy = pltpu.make_async_copy(hbm_ref, out_ref, sem)
    copy.start()
    copy.wait()


def load(x):
    return pl.pallas_call(
        load_kernel,
        in_specs=[pl.BlockSpec(memory_space=pltpu.HBM)],
        out_specs=pl.BlockSpec(memory_space=pltpu.VMEM),
        out_shape=pltpu.VMEM(x.shape, x.dtype),
        scratch_shapes=[pltpu.SemaphoreType.DMA],
        compiler_params=pltpu.CompilerParams(vmem_limit_bytes=1024 * 1024 + 2 * x.size),
        cost_estimate=pl.CostEstimate(flops=4000000, bytes_accessed=2 * x.size, transcendentals=0),
        name="load",
    )(in_hbm(x))


def query_kernel(nope_ref, absorb_ref, out_ref):
    for h in range(absorb_ref.shape[0]):
        out_ref[h] = jnp.dot(
            nope_ref[:, h * NOPE : (h + 1) * NOPE], absorb_ref[h], preferred_element_type=jnp.float32
        ).astype(jnp.bfloat16)


def queries(q_nope, w_uk):
    rows = q_nope.shape[0]
    head_count = w_uk.shape[0]
    vmem = pl.BlockSpec(memory_space=pltpu.VMEM)
    return pl.pallas_call(
        query_kernel,
        in_specs=[vmem, vmem],
        out_specs=vmem,
        out_shape=jax.ShapeDtypeStruct((head_count, rows, LATENT), jnp.bfloat16),
        compiler_params=pltpu.CompilerParams(vmem_limit_bytes=4 * 1024 * 1024),
        cost_estimate=pl.CostEstimate(
            flops=2 * head_count * rows * NOPE * LATENT, bytes_accessed=6 * 1024 * 1024, transcendentals=0
        ),
        name="queries",
    )(q_nope, w_uk)


def column_of(row):
    size = row.shape[1]
    across = lax.broadcasted_iota(jnp.int32, (size, size), 1)
    down = lax.broadcasted_iota(jnp.int32, (size, size), 0)
    return jnp.sum(jnp.where(across == down, row, 0), axis=1, keepdims=True)


def pack_kernel(pos_ref, nope_ref, rope_ref, *rest):
    out_refs, sems = rest[:-1], rest[-1]
    rows, wide = nope_ref.shape
    narrow = rope_ref.shape[1]
    copies = []
    for n, out_ref in enumerate(out_refs):
        part = pl.ds(rows - out_ref.shape[0], out_ref.shape[0])
        copies.append(pltpu.make_async_copy(nope_ref.at[part], out_ref.at[:, :wide], sems.at[2 * n]))
        copies.append(
            pltpu.make_async_copy(
                rope_ref.at[part], out_ref.at[:, wide : wide + narrow], sems.at[2 * n + 1]
            )
        )
    for copy in copies:
        copy.start()
    pos = column_of(pos_ref[...])
    lane = lax.broadcasted_iota(jnp.int32, (rows, 128), 1)
    coded = jnp.where(lane == 0, pos >> 8, jnp.where(lane == 1, pos & 255, 0))
    coded = coded.astype(jnp.float32).astype(jnp.bfloat16)
    for out_ref in out_refs:
        out_ref[:, wide + narrow :] = coded[rows - out_ref.shape[0] :]
    for copy in copies:
        copy.wait()


def pack(query_pos, q_nope, q_rope, sizes):
    rows, wide = q_nope.shape
    width = wide + q_rope.shape[1] + 128
    vmem = pl.BlockSpec(memory_space=pltpu.VMEM)
    hbm = pl.BlockSpec(memory_space=pltpu.HBM)
    return pl.pallas_call(
        pack_kernel,
        in_specs=[vmem, hbm, hbm],
        out_specs=[vmem] * len(sizes),
        out_shape=[jax.ShapeDtypeStruct((size, width), jnp.bfloat16) for size in sizes],
        scratch_shapes=[pltpu.SemaphoreType.DMA((2 * len(sizes),))],
        compiler_params=pltpu.CompilerParams(vmem_limit_bytes=2 * 1024 * 1024),
        cost_estimate=pl.CostEstimate(flops=1000000, bytes_accessed=2 * sum(sizes) * width, transcendentals=0),
        name="pack",
    )(query_pos.reshape(1, rows), in_hbm(q_nope), in_hbm(q_rope))


def assemble_kernel(*refs):
    tile_refs, out_ref = refs[:-1], refs[-1]
    half = tile_refs[0].shape[1]
    for t, tile_ref in enumerate(tile_refs):
        out_ref[:, t * half : (t + 1) * half] = tile_ref[...]


def assemble(tiles):
    depth, half = tiles[0].shape
    vmem = pl.BlockSpec(memory_space=pltpu.VMEM)
    return pl.pallas_call(
        assemble_kernel,
        in_specs=[vmem] * len(tiles),
        out_specs=vmem,
        out_shape=jax.ShapeDtypeStruct((depth, half * len(tiles)), jnp.bfloat16),
        compiler_params=pltpu.CompilerParams(vmem_limit_bytes=4 * 1024 * 1024),
        cost_estimate=pl.CostEstimate(
            flops=1000000, bytes_accessed=4 * depth * half * len(tiles), transcendentals=0
        ),
        name="assemble",
    )(*tiles)


exponent_scale = softmax_scale * 1.4426950408889634
lowest_start = -1e30


def visible(block_ref, limit, tiles):
    half = PANEL // 2
    my_row = lax.axis_index("row")
    side = lax.axis_index("head") & 1
    lane = lax.broadcasted_iota(jnp.int32, (1, half), 1)
    shown = []
    for k, other in tiles:
        start = block_ref[my_row ^ k] * PANEL + ((1 - side) if other else side) * half
        shown.append(start + lane <= limit)
    return shown


def masked_scores(latent, rope, keys, shown, rows):
    half = PANEL // 2
    scores = jnp.dot(jnp.concatenate((latent, rope), axis=1), keys, preferred_element_type=jnp.float32)
    group = scores.shape[0] // rows
    masked = []
    for t, mask in enumerate(shown):
        part = scores[:, t * half : (t + 1) * half].reshape(group, rows, half)
        masked.append(jnp.where(mask[None], part, -jnp.inf).reshape(group * rows, half))
    return jnp.concatenate(masked, axis=1)


def mix(weights, keys):
    return lax.dot_general(
        weights.astype(jnp.bfloat16), keys[:LATENT], (((1,), (1,)), ((), ())), preferred_element_type=jnp.float32
    )


def store_values(mixed, members, rows, up_ref, out_refs):
    for g, h in enumerate(members):
        value = jnp.dot(mixed[g * rows : (g + 1) * rows], up_ref[h], preferred_element_type=jnp.float32)
        value = value.astype(jnp.bfloat16)
        done = 0
        for out_ref in out_refs:
            size = out_ref.shape[0]
            out_ref[:, h * VHEAD : (h + 1) * VHEAD] = value[done : done + size]
            done += size


def head_groups(heads, rows):
    group = max(1, min(heads, 512 // rows))
    return [range(first, first + group) for first in range(0, heads, group)]


def stacked(part_of, members):
    return jnp.concatenate([part_of(h) for h in members], axis=0)


def all_tiles(columns):
    count = columns // PANEL
    return [(k, False) for k in range(count)] + [(k, True) for k in range(count)]


def attend(block_ref, limit, rows, latent_of, rope_of, up_ref, keys_ref, out_refs):
    shown = visible(block_ref, limit, all_tiles(keys_ref.shape[1]))
    for members in head_groups(up_ref.shape[0], rows):
        scores = masked_scores(
            stacked(latent_of, members), stacked(rope_of, members), keys_ref[...], shown, rows
        )
        top = jnp.max(scores, axis=1, keepdims=True)
        weights = jnp.exp2((scores - top) * exponent_scale)
        denominator = jnp.sum(weights, axis=1, keepdims=True)
        mixed = (mix(weights, keys_ref[...]) * (1.0 / denominator)).astype(jnp.bfloat16)
        store_values(mixed, members, rows, up_ref, out_refs)


def early_kernel(tiles, rows, block_ref, pos_ref, latent_ref, rope_ref, keys_ref, top_ref, sum_ref, mix_ref):
    shown = visible(block_ref, column_of(pos_ref[...])[:rows], tiles)
    for members in head_groups(latent_ref.shape[0], rows):
        scores = masked_scores(
            stacked(lambda h: latent_ref[h, :rows], members),
            stacked(lambda h: rope_ref[:rows, h * ROPE : (h + 1) * ROPE], members),
            keys_ref[...],
            shown,
            rows,
        )
        top = jnp.maximum(jnp.max(scores, axis=1, keepdims=True), lowest_start)
        weights = jnp.exp2((scores - top) * exponent_scale)
        at = slice(members[0] * rows, (members[-1] + 1) * rows)
        top_ref[at] = top
        sum_ref[at] = jnp.sum(weights, axis=1, keepdims=True)
        mix_ref[at] = mix(weights, keys_ref[...])


def late_kernel(
    tiles, rows, block_ref, pos_ref, latent_ref, rope_ref, top_ref, sum_ref, mix_ref, *rest
):
    tile_refs, (up_ref, out_ref) = rest[: len(tiles)], rest[len(tiles) :]
    keys = jnp.concatenate([r[...] for r in tile_refs], axis=1)
    shown = visible(block_ref, column_of(pos_ref[...])[:rows], tiles)
    for members in head_groups(latent_ref.shape[0], rows):
        scores = masked_scores(
            stacked(lambda h: latent_ref[h, :rows], members),
            stacked(lambda h: rope_ref[:rows, h * ROPE : (h + 1) * ROPE], members),
            keys,
            shown,
            rows,
        )
        at = slice(members[0] * rows, (members[-1] + 1) * rows)
        top = jnp.maximum(jnp.max(scores, axis=1, keepdims=True), top_ref[at])
        weights = jnp.exp2((scores - top) * exponent_scale)
        before = jnp.exp2((top_ref[at] - top) * exponent_scale)
        denominator = jnp.sum(weights, axis=1, keepdims=True) + sum_ref[at] * before
        share = 1.0 / denominator
        mixed = mix(weights, keys) * share + mix_ref[at] * (before * share)
        store_values(mixed.astype(jnp.bfloat16), members, rows, up_ref, [out_ref])


def early_attention(tiles, rows, panel_block, pos, query_latent, q_rope, keys):
    head_count = query_latent.shape[0]
    depth, columns = keys.shape
    count = head_count * rows
    vmem = pl.BlockSpec(memory_space=pltpu.VMEM)
    return pl.pallas_call(
        functools.partial(early_kernel, tiles, rows),
        in_specs=[pl.BlockSpec(memory_space=pltpu.SMEM)] + [vmem] * 4,
        out_specs=[vmem] * 3,
        out_shape=[jax.ShapeDtypeStruct((count, size), jnp.float32) for size in (1, 1, LATENT)],
        compiler_params=pltpu.CompilerParams(vmem_limit_bytes=12 * 1024 * 1024),
        cost_estimate=pl.CostEstimate(
            flops=2 * count * columns * (depth + LATENT),
            bytes_accessed=4 * 1024 * 1024,
            transcendentals=count * columns,
        ),
        name="early_attention",
    )(panel_block, pos, query_latent, q_rope, keys)


def late_attention(tiles, rows, panel_block, pos, query_latent, q_rope, early, arrays, w_uv):
    head_count = query_latent.shape[0]
    depth, columns = arrays[0].shape
    count = head_count * rows
    vmem = pl.BlockSpec(memory_space=pltpu.VMEM)
    return pl.pallas_call(
        functools.partial(late_kernel, tiles, rows),
        in_specs=[pl.BlockSpec(memory_space=pltpu.SMEM)] + [vmem] * (7 + len(arrays)),
        out_specs=vmem,
        out_shape=jax.ShapeDtypeStruct((rows, head_count * VHEAD), jnp.bfloat16),
        compiler_params=pltpu.CompilerParams(vmem_limit_bytes=12 * 1024 * 1024),
        cost_estimate=pl.CostEstimate(
            flops=2 * count * (columns * len(arrays) * (depth + LATENT) + LATENT * VHEAD),
            bytes_accessed=4 * 1024 * 1024,
            transcendentals=count * columns * len(arrays),
        ),
        name="late_attention",
    )(panel_block, pos, query_latent, q_rope, *early, *arrays, w_uv)


def own_kernel(first, rows, block_ref, pos_ref, latent_ref, rope_ref, up_ref, keys_ref, *rest):
    part = slice(first, first + rows)
    copy = None
    out_refs = rest
    if first:
        w_ref, out_refs, held_ref, sem = rest[0], rest[1:-2], rest[-2], rest[-1]
        copy = pltpu.make_async_copy(w_ref, held_ref, sem)
        copy.start()
    attend(
        block_ref,
        column_of(pos_ref[...])[part],
        rows,
        lambda h: latent_ref[h, part],
        lambda h: rope_ref[part, h * ROPE : (h + 1) * ROPE],
        up_ref,
        keys_ref,
        out_refs,
    )
    if copy is not None:
        copy.wait()


def packed_kernel(block_ref, packed_ref, absorb_ref, up_ref, keys_ref, *out_refs):
    rows = packed_ref.shape[0]
    heads = up_ref.shape[0]
    wide = heads * NOPE
    coded = packed_ref[:, wide + heads * ROPE :].astype(jnp.float32)
    limit = (coded[:, 0:1] * 256.0 + coded[:, 1:2]).astype(jnp.int32)
    attend(
        block_ref,
        limit,
        rows,
        lambda h: jnp.dot(
            packed_ref[:, h * NOPE : (h + 1) * NOPE], absorb_ref[h], preferred_element_type=jnp.float32
        ).astype(jnp.bfloat16),
        lambda h: packed_ref[:, wide + h * ROPE : wide + (h + 1) * ROPE],
        up_ref,
        keys_ref,
        out_refs,
    )


def attention(kernel, sizes, panel_block, *arrays, held=None):
    head_count = arrays[-2].shape[0]
    depth, cache = arrays[-1].shape
    rows = sum(sizes)
    flops = 2 * head_count * rows * (cache * (depth + LATENT) + LATENT * VHEAD)
    vmem = pl.BlockSpec(memory_space=pltpu.VMEM)
    more = [] if held is None else [held]
    return pl.pallas_call(
        kernel,
        in_specs=[pl.BlockSpec(memory_space=pltpu.SMEM)]
        + [vmem] * len(arrays)
        + [pl.BlockSpec(memory_space=pltpu.HBM)] * len(more),
        out_specs=[vmem] * (len(sizes) + len(more)),
        out_shape=[jax.ShapeDtypeStruct((size, head_count * VHEAD), jnp.bfloat16) for size in sizes]
        + [pltpu.VMEM(x.shape, x.dtype) for x in more],
        scratch_shapes=[pltpu.SemaphoreType.DMA] * len(more),
        compiler_params=pltpu.CompilerParams(vmem_limit_bytes=16 * 1024 * 1024),
        cost_estimate=pl.CostEstimate(
            flops=flops, bytes_accessed=8 * 1024 * 1024, transcendentals=head_count * rows * cache
        ),
        name="attention",
    )(panel_block, *arrays, *(in_hbm(x) for x in more))


def project_kernel(sub, parts, blocks, *refs):
    values_refs, (w_ref, sent_ref, kept_ref) = refs[:parts], refs[parts:]
    upper = (lax.axis_index("head") & 1) == 1
    features = w_ref.shape[0]
    tiles = [slice(first, min(first + 256, features)) for first in range(0, features, 256)]
    values = jnp.concatenate([r[...] for r in values_refs], axis=0) if parts > 1 else values_refs[0][...]
    for tile in tiles:
        product = lax.dot_general(
            values, w_ref[tile], (((1,), (1,)), ((), ())), preferred_element_type=jnp.float32
        )
        pairs = product.reshape(blocks, -1, 2, sub, product.shape[1])
        kept_ref[:, :, :, tile] = jnp.where(upper, pairs[:, :, 1], pairs[:, :, 0])
        sent_ref[:, :, :, tile] = jnp.where(upper, pairs[:, :, 0], pairs[:, :, 1]).astype(jnp.bfloat16)


def project(blocks, w_out, sub):
    parts = [chunk for block in blocks for chunk in block]
    rows = sum(chunk.shape[0] for chunk in blocks[0])
    features, depth = w_out.shape
    shape = (len(blocks), rows // (2 * sub), sub, features)
    vmem = pl.BlockSpec(memory_space=pltpu.VMEM)
    return pl.pallas_call(
        functools.partial(project_kernel, sub, len(parts), len(blocks)),
        in_specs=[vmem] * (len(parts) + 1),
        out_specs=[vmem, vmem],
        compiler_params=pltpu.CompilerParams(vmem_limit_bytes=(1 + len(blocks)) * 1024 * 1024),
        out_shape=[jax.ShapeDtypeStruct(shape, jnp.bfloat16), jax.ShapeDtypeStruct(shape, jnp.float32)],
        cost_estimate=pl.CostEstimate(
            flops=2 * len(blocks) * rows * depth * features,
            bytes_accessed=2 * depth * (features + rows),
            transcendentals=0,
        ),
        name="project",
    )(*parts, w_out)


def pair_kernel(parts, *refs):
    kept_refs, come_refs, out_refs = refs[:parts], refs[parts : 2 * parts], refs[2 * parts :]
    chip = lax.axis_index("head") >> 1
    for j, out_ref in enumerate(out_refs):
        done = 0
        for kept_ref, come_ref in zip(kept_refs, come_refs):
            at = pl.ds(chip ^ j, 1)
            total = kept_ref[:, at] + come_ref[:, at].astype(jnp.float32)
            blocks = total.shape[0]
            out_ref[done : done + blocks] = total[:, 0].astype(out_ref.dtype)
            done += blocks


def pair_sum(kept, come):
    _, count, sub, features = kept[0].shape
    blocks = sum(k.shape[0] for k in kept)
    vmem = pl.BlockSpec(memory_space=pltpu.VMEM)
    return pl.pallas_call(
        functools.partial(pair_kernel, len(kept)),
        in_specs=[vmem] * (2 * len(kept)),
        out_specs=[vmem] * count,
        compiler_params=pltpu.CompilerParams(vmem_limit_bytes=2 * 1024 * 1024),
        out_shape=[
            jax.ShapeDtypeStruct((blocks, sub, features), jnp.bfloat16 if j else jnp.float32)
            for j in range(count)
        ],
        cost_estimate=pl.CostEstimate(
            flops=blocks * count * sub * features,
            bytes_accessed=6 * blocks * count * sub * features,
            transcendentals=0,
        ),
        name="pair_sum",
    )(*kept, *come)


def chip_kernel(*refs):
    count = refs[0].shape[0]
    terms, outs = refs[:-count], refs[-count:]
    for b, out_ref in enumerate(outs):
        total = terms[0][b]
        for term in terms[1:]:
            total = total + term[b].astype(jnp.float32)
        out_ref[...] = total.astype(jnp.bfloat16)


def chip_sum(terms):
    blocks, sub, features = terms[0].shape
    vmem = pl.BlockSpec(memory_space=pltpu.VMEM)
    return pl.pallas_call(
        chip_kernel,
        in_specs=[vmem] * len(terms),
        out_specs=[vmem] * blocks,
        compiler_params=pltpu.CompilerParams(vmem_limit_bytes=2 * 1024 * 1024),
        out_shape=[jax.ShapeDtypeStruct((sub, features), jnp.bfloat16)] * blocks,
        cost_estimate=pl.CostEstimate(
            flops=len(terms) * blocks * sub * features,
            bytes_accessed=2 * len(terms) * blocks * sub * features,
            transcendentals=0,
        ),
        name="chip_sum",
    )(*terms)


def finish_kernel(*refs):
    pieces, out_ref = refs[:-1], refs[-1]
    width = pieces[0].shape[1]
    my_row = lax.axis_index("row")
    for k, piece_ref in enumerate(pieces):
        columns = pl.ds(pl.multiple_of((my_row ^ k) * width, width), width)
        out_ref[:, columns] = piece_ref[...]


def finish(pieces):
    sub, width = pieces[0].shape
    if width % 128:
        out = jnp.zeros((sub, width * len(pieces)), jnp.bfloat16)
        for k, piece in enumerate(pieces):
            out = lax.dynamic_update_slice(out, piece, (0, (lax.axis_index("row") ^ k) * width))
        return out
    vmem = pl.BlockSpec(memory_space=pltpu.VMEM)
    return pl.pallas_call(
        finish_kernel,
        in_specs=[vmem] * len(pieces),
        out_specs=vmem,
        compiler_params=pltpu.CompilerParams(vmem_limit_bytes=2 * 1024 * 1024),
        out_shape=jax.ShapeDtypeStruct((sub, width * len(pieces)), jnp.bfloat16),
        name="finish",
    )(*pieces)


def on_device(q_nope, q_rope, latent_keys, rope_keys, panel_block, query_pos, w_uk, w_uv, w_out):
    row_devices = lax.axis_size("row")
    sub_rows = q_nope.shape[0] // lax.axis_size("head")

    mine = panel_half(latent_keys, rope_keys)
    halves = [block[0] for block in gather_blocks([mine])]
    others = []
    for h in halves:
        others.append(swap(h, "head", 1))
    rows = q_nope.shape[0]
    w_uk = load(w_uk)
    query_latent = queries(q_nope, w_uk)
    (packed,) = pack(query_pos, q_nope, q_rope, [rows // 2])
    w_uv = load(w_uv)
    packed = swap(packed, "row", 1)
    pos = query_pos.reshape(1, rows)
    last = row_devices - 1
    tiles = all_tiles(row_devices * PANEL)
    first_tiles = [t for t in tiles if t[0] != last]
    last_tiles = [t for t in tiles if t[0] == last]
    arrays_of = lambda some: [others[k] if other else halves[k] for k, other in some]
    early = early_attention(
        first_tiles, rows // 2, panel_block, pos, query_latent, q_rope, assemble(arrays_of(first_tiles))
    )
    chunks = [
        late_attention(
            last_tiles, rows // 2, panel_block, pos, query_latent, q_rope, early, arrays_of(last_tiles), w_uv
        )
    ]
    keys = assemble(arrays_of(tiles))
    *more, w_out = attention(
        functools.partial(own_kernel, rows // 2, rows // 2),
        [rows // 4, rows // 4],
        panel_block,
        pos,
        query_latent,
        q_rope,
        w_uv,
        keys,
        held=w_out,
    )
    chunks += more
    guests = attention(packed_kernel, [rows // 4, rows // 4], panel_block, packed, w_uk, w_uv, keys)

    blocks = gather_blocks(chunks, {1: guests})
    pieces = []
    groups = [[[0], list(range(1, last))], [[last]]]
    for group in groups:
        kept, come = [], []
        for part in group:
            sent, stays = project([blocks[k] for k in part], w_out, sub_rows)
            come.append(swap(sent, "head", 1))
            kept.append(stays)
        sums = pair_sum(kept, come)
        terms = [sums[0]]
        for j in range(1, len(sums)):
            terms.append(swap(sums[j], "head", 2 * j))
        for k, total in zip(sum(group, []), chip_sum(terms)):
            pieces.append(swap(total, "row", k) if k else total)
    return finish(pieces)


def solution(mesh):
    return jax.shard_map(
        on_device,
        mesh=mesh,
        in_specs=(
            P("row", "head"),
            P("row", "head"),
            P(None, "row"),
            P(None, "row"),
            P(),
            P("row"),
            P("head", None, None),
            P("head", None, None),
            P("row", "head"),
        ),
        out_specs=P(("row", "head"), None),
        check_vma=False,
    )
```

```python
import functools

import jax
import jax.numpy as jnp
from jax import lax
from jax.experimental import pallas as pl
from jax.experimental.pallas import tpu as pltpu
from jax.sharding import PartitionSpec as P


NOPE = 128
ROPE = 64
LATENT = 512
VHEAD = 128
PANEL = 256


softmax_scale = 192.0 ** (-0.5)


def in_hbm(x):
    return pltpu.with_memory_space_constraint(x, pltpu.HBM)


def swap(x, axis, mask):
    count = lax.axis_size(axis)
    return lax.ppermute(x, axis, [(i, i ^ mask) for i in range(count)])


def gather_blocks(own, made=None):
    made = made or {}
    count = lax.axis_size("row")
    blocks = {0: own}
    mask = count // 2
    while mask:
        for k in list(blocks):
            known = list(made.get(mask, ())) if k == 0 else []
            moved = []
            for chunk in blocks[k][: len(blocks[k]) - len(known)]:
                moved.append(swap(chunk, "row", mask))
            blocks[k ^ mask] = moved + known
        mask //= 2
    return [blocks[k] for k in range(count)]


def half_kernel(latent_ref, rope_ref, out_ref, sems):
    half = out_ref.shape[1]
    side = lax.axis_index("head") & 1
    columns = pl.ds(pl.multiple_of(side * half, half), half)
    latent = pltpu.make_async_copy(latent_ref.at[:, columns], out_ref.at[:LATENT], sems.at[0])
    rope = pltpu.make_async_copy(rope_ref.at[:, columns], out_ref.at[LATENT:], sems.at[1])
    latent.start()
    rope.start()
    latent.wait()
    rope.wait()


def panel_half(latent_keys, rope_keys):
    half = latent_keys.shape[1] // 2
    depth = LATENT + ROPE
    whole = pl.BlockSpec(memory_space=pltpu.HBM)
    return pl.pallas_call(
        half_kernel,
        in_specs=[whole, whole],
        out_specs=pl.BlockSpec(memory_space=pltpu.VMEM),
        out_shape=jax.ShapeDtypeStruct((depth, half), jnp.bfloat16),
        scratch_shapes=[pltpu.SemaphoreType.DMA((2,))],
        compiler_params=pltpu.CompilerParams(vmem_limit_bytes=2 * 1024 * 1024),
        cost_estimate=pl.CostEstimate(flops=1000000, bytes_accessed=4 * depth * half, transcendentals=0),
        name="panel_half",
    )(in_hbm(latent_keys), in_hbm(rope_keys))


def load_kernel(hbm_ref, out_ref, sem):
    copy = pltpu.make_async_copy(hbm_ref, out_ref, sem)
    copy.start()
    copy.wait()


def load(x):
    return pl.pallas_call(
        load_kernel,
        in_specs=[pl.BlockSpec(memory_space=pltpu.HBM)],
        out_specs=pl.BlockSpec(memory_space=pltpu.VMEM),
        out_shape=pltpu.VMEM(x.shape, x.dtype),
        scratch_shapes=[pltpu.SemaphoreType.DMA],
        compiler_params=pltpu.CompilerParams(vmem_limit_bytes=1024 * 1024 + 2 * x.size),
        cost_estimate=pl.CostEstimate(flops=4000000, bytes_accessed=2 * x.size, transcendentals=0),
        name="load",
    )(in_hbm(x))


def query_kernel(nope_ref, absorb_ref, out_ref):
    for h in range(absorb_ref.shape[0]):
        out_ref[h] = jnp.dot(
            nope_ref[:, h * NOPE : (h + 1) * NOPE], absorb_ref[h], preferred_element_type=jnp.float32
        ).astype(jnp.bfloat16)


def queries(q_nope, w_uk):
    rows = q_nope.shape[0]
    head_count = w_uk.shape[0]
    vmem = pl.BlockSpec(memory_space=pltpu.VMEM)
    return pl.pallas_call(
        query_kernel,
        in_specs=[vmem, vmem],
        out_specs=vmem,
        out_shape=jax.ShapeDtypeStruct((head_count, rows, LATENT), jnp.bfloat16),
        compiler_params=pltpu.CompilerParams(vmem_limit_bytes=4 * 1024 * 1024),
        cost_estimate=pl.CostEstimate(
            flops=2 * head_count * rows * NOPE * LATENT, bytes_accessed=6 * 1024 * 1024, transcendentals=0
        ),
        name="queries",
    )(q_nope, w_uk)


def column_of(row):
    size = row.shape[1]
    across = lax.broadcasted_iota(jnp.int32, (size, size), 1)
    down = lax.broadcasted_iota(jnp.int32, (size, size), 0)
    return jnp.sum(jnp.where(across == down, row, 0), axis=1, keepdims=True)


def pack_kernel(pos_ref, nope_ref, rope_ref, *rest):
    out_refs, sems = rest[:-1], rest[-1]
    rows, wide = nope_ref.shape
    narrow = rope_ref.shape[1]
    copies = []
    for n, out_ref in enumerate(out_refs):
        part = pl.ds(rows - out_ref.shape[0], out_ref.shape[0])
        copies.append(pltpu.make_async_copy(nope_ref.at[part], out_ref.at[:, :wide], sems.at[2 * n]))
        copies.append(
            pltpu.make_async_copy(
                rope_ref.at[part], out_ref.at[:, wide : wide + narrow], sems.at[2 * n + 1]
            )
        )
    for copy in copies:
        copy.start()
    pos = column_of(pos_ref[...])
    lane = lax.broadcasted_iota(jnp.int32, (rows, 128), 1)
    coded = jnp.where(lane == 0, pos >> 8, jnp.where(lane == 1, pos & 255, 0))
    coded = coded.astype(jnp.float32).astype(jnp.bfloat16)
    for out_ref in out_refs:
        out_ref[:, wide + narrow :] = coded[rows - out_ref.shape[0] :]
    for copy in copies:
        copy.wait()


def pack(query_pos, q_nope, q_rope, sizes):
    rows, wide = q_nope.shape
    width = wide + q_rope.shape[1] + 128
    vmem = pl.BlockSpec(memory_space=pltpu.VMEM)
    hbm = pl.BlockSpec(memory_space=pltpu.HBM)
    return pl.pallas_call(
        pack_kernel,
        in_specs=[vmem, hbm, hbm],
        out_specs=[vmem] * len(sizes),
        out_shape=[jax.ShapeDtypeStruct((size, width), jnp.bfloat16) for size in sizes],
        scratch_shapes=[pltpu.SemaphoreType.DMA((2 * len(sizes),))],
        compiler_params=pltpu.CompilerParams(vmem_limit_bytes=2 * 1024 * 1024),
        cost_estimate=pl.CostEstimate(flops=1000000, bytes_accessed=2 * sum(sizes) * width, transcendentals=0),
        name="pack",
    )(query_pos.reshape(1, rows), in_hbm(q_nope), in_hbm(q_rope))


def assemble_kernel(*refs):
    tile_refs, out_ref = refs[:-1], refs[-1]
    half = tile_refs[0].shape[1]
    for t, tile_ref in enumerate(tile_refs):
        out_ref[:, t * half : (t + 1) * half] = tile_ref[...]


def assemble(tiles):
    depth, half = tiles[0].shape
    vmem = pl.BlockSpec(memory_space=pltpu.VMEM)
    return pl.pallas_call(
        assemble_kernel,
        in_specs=[vmem] * len(tiles),
        out_specs=vmem,
        out_shape=jax.ShapeDtypeStruct((depth, half * len(tiles)), jnp.bfloat16),
        compiler_params=pltpu.CompilerParams(vmem_limit_bytes=4 * 1024 * 1024),
        cost_estimate=pl.CostEstimate(
            flops=1000000, bytes_accessed=4 * depth * half * len(tiles), transcendentals=0
        ),
        name="assemble",
    )(*tiles)


exponent_scale = softmax_scale * 1.4426950408889634
lowest_start = -1e30


def visible(block_ref, limit, tiles):
    half = PANEL // 2
    my_row = lax.axis_index("row")
    side = lax.axis_index("head") & 1
    lane = lax.broadcasted_iota(jnp.int32, (1, half), 1)
    shown = []
    for k, other in tiles:
        start = block_ref[my_row ^ k] * PANEL + ((1 - side) if other else side) * half
        shown.append(start + lane <= limit)
    return shown


def masked_scores(latent, rope, keys, shown, rows):
    half = PANEL // 2
    scores = jnp.dot(jnp.concatenate((latent, rope), axis=1), keys, preferred_element_type=jnp.float32)
    group = scores.shape[0] // rows
    masked = []
    for t, mask in enumerate(shown):
        part = scores[:, t * half : (t + 1) * half].reshape(group, rows, half)
        masked.append(jnp.where(mask[None], part, -jnp.inf).reshape(group * rows, half))
    return jnp.concatenate(masked, axis=1)


def mix(weights, keys):
    return lax.dot_general(
        weights.astype(jnp.bfloat16), keys[:LATENT], (((1,), (1,)), ((), ())), preferred_element_type=jnp.float32
    )


def store_values(mixed, members, rows, up_ref, out_refs):
    for g, h in enumerate(members):
        value = jnp.dot(mixed[g * rows : (g + 1) * rows], up_ref[h], preferred_element_type=jnp.float32)
        value = value.astype(jnp.bfloat16)
        done = 0
        for out_ref in out_refs:
            size = out_ref.shape[0]
            out_ref[:, h * VHEAD : (h + 1) * VHEAD] = value[done : done + size]
            done += size


def head_groups(heads, rows):
    group = max(1, min(heads, 512 // rows))
    return [range(first, first + group) for first in range(0, heads, group)]


def stacked(part_of, members):
    return jnp.concatenate([part_of(h) for h in members], axis=0)


def all_tiles(columns):
    count = columns // PANEL
    return [(k, False) for k in range(count)] + [(k, True) for k in range(count)]


def attend(block_ref, limit, rows, latent_of, rope_of, up_ref, keys_ref, out_refs):
    shown = visible(block_ref, limit, all_tiles(keys_ref.shape[1]))
    for members in head_groups(up_ref.shape[0], rows):
        scores = masked_scores(
            stacked(latent_of, members), stacked(rope_of, members), keys_ref[...], shown, rows
        )
        top = jnp.max(scores, axis=1, keepdims=True)
        weights = jnp.exp2((scores - top) * exponent_scale)
        denominator = jnp.sum(weights, axis=1, keepdims=True)
        mixed = (mix(weights, keys_ref[...]) * (1.0 / denominator)).astype(jnp.bfloat16)
        store_values(mixed, members, rows, up_ref, out_refs)


def early_kernel(tiles, rows, block_ref, pos_ref, latent_ref, rope_ref, keys_ref, top_ref, sum_ref, mix_ref):
    shown = visible(block_ref, column_of(pos_ref[...])[:rows], tiles)
    for members in head_groups(latent_ref.shape[0], rows):
        scores = masked_scores(
            stacked(lambda h: latent_ref[h, :rows], members),
            stacked(lambda h: rope_ref[:rows, h * ROPE : (h + 1) * ROPE], members),
            keys_ref[...],
            shown,
            rows,
        )
        top = jnp.maximum(jnp.max(scores, axis=1, keepdims=True), lowest_start)
        weights = jnp.exp2((scores - top) * exponent_scale)
        at = slice(members[0] * rows, (members[-1] + 1) * rows)
        top_ref[at] = top
        sum_ref[at] = jnp.sum(weights, axis=1, keepdims=True)
        mix_ref[at] = mix(weights, keys_ref[...])


def late_kernel(
    tiles, rows, block_ref, pos_ref, latent_ref, rope_ref, top_ref, sum_ref, mix_ref, *rest
):
    tile_refs, (up_ref, out_ref) = rest[: len(tiles)], rest[len(tiles) :]
    keys = jnp.concatenate([r[...] for r in tile_refs], axis=1)
    shown = visible(block_ref, column_of(pos_ref[...])[:rows], tiles)
    for members in head_groups(latent_ref.shape[0], rows):
        scores = masked_scores(
            stacked(lambda h: latent_ref[h, :rows], members),
            stacked(lambda h: rope_ref[:rows, h * ROPE : (h + 1) * ROPE], members),
            keys,
            shown,
            rows,
        )
        at = slice(members[0] * rows, (members[-1] + 1) * rows)
        top = jnp.maximum(jnp.max(scores, axis=1, keepdims=True), top_ref[at])
        weights = jnp.exp2((scores - top) * exponent_scale)
        before = jnp.exp2((top_ref[at] - top) * exponent_scale)
        denominator = jnp.sum(weights, axis=1, keepdims=True) + sum_ref[at] * before
        share = 1.0 / denominator
        mixed = mix(weights, keys) * share + mix_ref[at] * (before * share)
        store_values(mixed.astype(jnp.bfloat16), members, rows, up_ref, [out_ref])


def early_attention(tiles, rows, panel_block, pos, query_latent, q_rope, keys):
    head_count = query_latent.shape[0]
    depth, columns = keys.shape
    count = head_count * rows
    vmem = pl.BlockSpec(memory_space=pltpu.VMEM)
    return pl.pallas_call(
        functools.partial(early_kernel, tiles, rows),
        in_specs=[pl.BlockSpec(memory_space=pltpu.SMEM)] + [vmem] * 4,
        out_specs=[vmem] * 3,
        out_shape=[jax.ShapeDtypeStruct((count, size), jnp.float32) for size in (1, 1, LATENT)],
        compiler_params=pltpu.CompilerParams(vmem_limit_bytes=12 * 1024 * 1024),
        cost_estimate=pl.CostEstimate(
            flops=2 * count * columns * (depth + LATENT),
            bytes_accessed=4 * 1024 * 1024,
            transcendentals=count * columns,
        ),
        name="early_attention",
    )(panel_block, pos, query_latent, q_rope, keys)


def late_attention(tiles, rows, panel_block, pos, query_latent, q_rope, early, arrays, w_uv):
    head_count = query_latent.shape[0]
    depth, columns = arrays[0].shape
    count = head_count * rows
    vmem = pl.BlockSpec(memory_space=pltpu.VMEM)
    return pl.pallas_call(
        functools.partial(late_kernel, tiles, rows),
        in_specs=[pl.BlockSpec(memory_space=pltpu.SMEM)] + [vmem] * (7 + len(arrays)),
        out_specs=vmem,
        out_shape=jax.ShapeDtypeStruct((rows, head_count * VHEAD), jnp.bfloat16),
        compiler_params=pltpu.CompilerParams(vmem_limit_bytes=12 * 1024 * 1024),
        cost_estimate=pl.CostEstimate(
            flops=2 * count * (columns * len(arrays) * (depth + LATENT) + LATENT * VHEAD),
            bytes_accessed=4 * 1024 * 1024,
            transcendentals=count * columns * len(arrays),
        ),
        name="late_attention",
    )(panel_block, pos, query_latent, q_rope, *early, *arrays, w_uv)


def own_kernel(first, rows, block_ref, pos_ref, latent_ref, rope_ref, up_ref, keys_ref, *rest):
    part = slice(first, first + rows)
    copy = None
    out_refs = rest
    if first:
        w_ref, out_refs, held_ref, sem = rest[0], rest[1:-2], rest[-2], rest[-1]
        copy = pltpu.make_async_copy(w_ref, held_ref, sem)
        copy.start()
    attend(
        block_ref,
        column_of(pos_ref[...])[part],
        rows,
        lambda h: latent_ref[h, part],
        lambda h: rope_ref[part, h * ROPE : (h + 1) * ROPE],
        up_ref,
        keys_ref,
        out_refs,
    )
    if copy is not None:
        copy.wait()


def packed_kernel(block_ref, packed_ref, absorb_ref, up_ref, keys_ref, *out_refs):
    rows = packed_ref.shape[0]
    heads = up_ref.shape[0]
    wide = heads * NOPE
    coded = packed_ref[:, wide + heads * ROPE :].astype(jnp.float32)
    limit = (coded[:, 0:1] * 256.0 + coded[:, 1:2]).astype(jnp.int32)
    attend(
        block_ref,
        limit,
        rows,
        lambda h: jnp.dot(
            packed_ref[:, h * NOPE : (h + 1) * NOPE], absorb_ref[h], preferred_element_type=jnp.float32
        ).astype(jnp.bfloat16),
        lambda h: packed_ref[:, wide + h * ROPE : wide + (h + 1) * ROPE],
        up_ref,
        keys_ref,
        out_refs,
    )


def attention(kernel, sizes, panel_block, *arrays, held=None):
    head_count = arrays[-2].shape[0]
    depth, cache = arrays[-1].shape
    rows = sum(sizes)
    flops = 2 * head_count * rows * (cache * (depth + LATENT) + LATENT * VHEAD)
    vmem = pl.BlockSpec(memory_space=pltpu.VMEM)
    more = [] if held is None else [held]
    return pl.pallas_call(
        kernel,
        in_specs=[pl.BlockSpec(memory_space=pltpu.SMEM)]
        + [vmem] * len(arrays)
        + [pl.BlockSpec(memory_space=pltpu.HBM)] * len(more),
        out_specs=[vmem] * (len(sizes) + len(more)),
        out_shape=[jax.ShapeDtypeStruct((size, head_count * VHEAD), jnp.bfloat16) for size in sizes]
        + [pltpu.VMEM(x.shape, x.dtype) for x in more],
        scratch_shapes=[pltpu.SemaphoreType.DMA] * len(more),
        compiler_params=pltpu.CompilerParams(vmem_limit_bytes=16 * 1024 * 1024),
        cost_estimate=pl.CostEstimate(
            flops=flops, bytes_accessed=8 * 1024 * 1024, transcendentals=head_count * rows * cache
        ),
        name="attention",
    )(panel_block, *arrays, *(in_hbm(x) for x in more))


def project_kernel(sub, parts, blocks, *refs):
    values_refs, (w_ref, sent_ref, kept_ref) = refs[:parts], refs[parts:]
    upper = (lax.axis_index("head") & 1) == 1
    features = w_ref.shape[0]
    tiles = [slice(first, min(first + 256, features)) for first in range(0, features, 256)]
    values = jnp.concatenate([r[...] for r in values_refs], axis=0) if parts > 1 else values_refs[0][...]
    for tile in tiles:
        product = lax.dot_general(
            values, w_ref[tile], (((1,), (1,)), ((), ())), preferred_element_type=jnp.float32
        )
        pairs = product.reshape(blocks, -1, 2, sub, product.shape[1])
        kept_ref[:, :, :, tile] = jnp.where(upper, pairs[:, :, 1], pairs[:, :, 0])
        sent_ref[:, :, :, tile] = jnp.where(upper, pairs[:, :, 0], pairs[:, :, 1]).astype(jnp.bfloat16)


def project(blocks, w_out, sub):
    parts = [chunk for block in blocks for chunk in block]
    rows = sum(chunk.shape[0] for chunk in blocks[0])
    features, depth = w_out.shape
    shape = (len(blocks), rows // (2 * sub), sub, features)
    vmem = pl.BlockSpec(memory_space=pltpu.VMEM)
    return pl.pallas_call(
        functools.partial(project_kernel, sub, len(parts), len(blocks)),
        in_specs=[vmem] * (len(parts) + 1),
        out_specs=[vmem, vmem],
        compiler_params=pltpu.CompilerParams(vmem_limit_bytes=(1 + len(blocks)) * 1024 * 1024),
        out_shape=[jax.ShapeDtypeStruct(shape, jnp.bfloat16), jax.ShapeDtypeStruct(shape, jnp.float32)],
        cost_estimate=pl.CostEstimate(
            flops=2 * len(blocks) * rows * depth * features,
            bytes_accessed=2 * depth * (features + rows),
            transcendentals=0,
        ),
        name="project",
    )(*parts, w_out)


def pair_kernel(parts, *refs):
    kept_refs, come_refs, out_refs = refs[:parts], refs[parts : 2 * parts], refs[2 * parts :]
    chip = lax.axis_index("head") >> 1
    for j, out_ref in enumerate(out_refs):
        done = 0
        for kept_ref, come_ref in zip(kept_refs, come_refs):
            at = pl.ds(chip ^ j, 1)
            total = kept_ref[:, at] + come_ref[:, at].astype(jnp.float32)
            blocks = total.shape[0]
            out_ref[done : done + blocks] = total[:, 0].astype(out_ref.dtype)
            done += blocks


def pair_sum(kept, come):
    _, count, sub, features = kept[0].shape
    blocks = sum(k.shape[0] for k in kept)
    vmem = pl.BlockSpec(memory_space=pltpu.VMEM)
    return pl.pallas_call(
        functools.partial(pair_kernel, len(kept)),
        in_specs=[vmem] * (2 * len(kept)),
        out_specs=[vmem] * count,
        compiler_params=pltpu.CompilerParams(vmem_limit_bytes=2 * 1024 * 1024),
        out_shape=[
            jax.ShapeDtypeStruct((blocks, sub, features), jnp.bfloat16 if j else jnp.float32)
            for j in range(count)
        ],
        cost_estimate=pl.CostEstimate(
            flops=blocks * count * sub * features,
            bytes_accessed=6 * blocks * count * sub * features,
            transcendentals=0,
        ),
        name="pair_sum",
    )(*kept, *come)


def chip_kernel(*refs):
    count = refs[0].shape[0]
    terms, outs = refs[:-count], refs[-count:]
    for b, out_ref in enumerate(outs):
        total = terms[0][b]
        for term in terms[1:]:
            total = total + term[b].astype(jnp.float32)
        out_ref[...] = total.astype(jnp.bfloat16)


def chip_sum(terms):
    blocks, sub, features = terms[0].shape
    vmem = pl.BlockSpec(memory_space=pltpu.VMEM)
    return pl.pallas_call(
        chip_kernel,
        in_specs=[vmem] * len(terms),
        out_specs=[vmem] * blocks,
        compiler_params=pltpu.CompilerParams(vmem_limit_bytes=2 * 1024 * 1024),
        out_shape=[jax.ShapeDtypeStruct((sub, features), jnp.bfloat16)] * blocks,
        cost_estimate=pl.CostEstimate(
            flops=len(terms) * blocks * sub * features,
            bytes_accessed=2 * len(terms) * blocks * sub * features,
            transcendentals=0,
        ),
        name="chip_sum",
    )(*terms)


def finish_kernel(*refs):
    pieces, out_ref = refs[:-1], refs[-1]
    width = pieces[0].shape[1]
    my_row = lax.axis_index("row")
    for k, piece_ref in enumerate(pieces):
        columns = pl.ds(pl.multiple_of((my_row ^ k) * width, width), width)
        out_ref[:, columns] = piece_ref[...]


def finish(pieces):
    sub, width = pieces[0].shape
    if width % 128:
        out = jnp.zeros((sub, width * len(pieces)), jnp.bfloat16)
        for k, piece in enumerate(pieces):
            out = lax.dynamic_update_slice(out, piece, (0, (lax.axis_index("row") ^ k) * width))
        return out
    vmem = pl.BlockSpec(memory_space=pltpu.VMEM)
    return pl.pallas_call(
        finish_kernel,
        in_specs=[vmem] * len(pieces),
        out_specs=vmem,
        compiler_params=pltpu.CompilerParams(vmem_limit_bytes=2 * 1024 * 1024),
        out_shape=jax.ShapeDtypeStruct((sub, width * len(pieces)), jnp.bfloat16),
        name="finish",
    )(*pieces)


def on_device(q_nope, q_rope, latent_keys, rope_keys, panel_block, query_pos, w_uk, w_uv, w_out):
    row_devices = lax.axis_size("row")
    sub_rows = q_nope.shape[0] // lax.axis_size("head")

    mine = panel_half(latent_keys, rope_keys)
    halves = [block[0] for block in gather_blocks([mine])]
    others = []
    for h in halves:
        others.append(swap(h, "head", 1))
    rows = q_nope.shape[0]
    w_uk = load(w_uk)
    query_latent = queries(q_nope, w_uk)
    (packed,) = pack(query_pos, q_nope, q_rope, [rows // 2])
    w_uv = load(w_uv)
    packed = swap(packed, "row", 1)
    pos = query_pos.reshape(1, rows)
    last = row_devices - 1
    tiles = all_tiles(row_devices * PANEL)
    early_panels = (0, 1)
    first_tiles = [t for t in tiles if t[0] in early_panels]
    last_tiles = [t for t in tiles if t[0] not in early_panels]
    arrays_of = lambda some: [others[k] if other else halves[k] for k, other in some]
    early = early_attention(
        first_tiles, rows // 2, panel_block, pos, query_latent, q_rope, assemble(arrays_of(first_tiles))
    )
    chunks = [
        late_attention(
            last_tiles, rows // 2, panel_block, pos, query_latent, q_rope, early, arrays_of(last_tiles), w_uv
        )
    ]
    keys = assemble(arrays_of(tiles))
    *more, w_out = attention(
        functools.partial(own_kernel, rows // 2, rows // 2),
        [rows // 4, rows // 4],
        panel_block,
        pos,
        query_latent,
        q_rope,
        w_uv,
        keys,
        held=w_out,
    )
    chunks += more
    guests = attention(packed_kernel, [rows // 4, rows // 4], panel_block, packed, w_uk, w_uv, keys)

    blocks = gather_blocks(chunks, {1: guests})
    pieces = []
    groups = [[[0], list(range(1, last))], [[last]]]
    for group in groups:
        kept, come = [], []
        for part in group:
            sent, stays = project([blocks[k] for k in part], w_out, sub_rows)
            come.append(swap(sent, "head", 1))
            kept.append(stays)
        sums = pair_sum(kept, come)
        terms = [sums[0]]
        for j in range(1, len(sums)):
            terms.append(swap(sums[j], "head", 2 * j))
        for k, total in zip(sum(group, []), chip_sum(terms)):
            pieces.append(swap(total, "row", k) if k else total)
    return finish(pieces)


def solution(mesh):
    return jax.shard_map(
        on_device,
        mesh=mesh,
        in_specs=(
            P("row", "head"),
            P("row", "head"),
            P(None, "row"),
            P(None, "row"),
            P(),
            P("row"),
            P("head", None, None),
            P("head", None, None),
            P("row", "head"),
        ),
        out_specs=P(("row", "head"), None),
        check_vma=False,
    )
```
